32 devices in a mesh: gene: 4 (over z), var: 4 (over y, core), perm: 2 (over x).
Axes of the slice: x: 2, y: 2, z: 4, core: 2. Of those that a mesh axis runs over, the one named last changes fastest.
Arguments:
- genotypes: bfloat16 [4, 6144, 768], P('gene', ('var', 'perm')), may hold values from 0 to 2
- phenotypes: float32 [512, 768], P('gene'), may hold values from -6 to 6
- perm_rows: int32 [256, 768], P(('var', 'perm')), may hold values from 0 to 767, each once within a row
- starts: int32 [512], P('gene'), may hold values from 0 to 2048, as said below
Outputs:
- maxima: float32 [256, 512], P(('var', 'perm'), 'gene')
- moments: float32 [2, 512], P(None, 'gene')
- pooled: float32 [2], replicated
The draws below stay inside these ranges and needn't reach their ends.
Inputs may be any that keep to these rules, and one draw needn't show every extreme that they name: `perm_rows`: each row is a permutation of 0 to 767. Within each block of 128 genes the starts never fall; a gene's window of 4096 variants lies inside its block's 6144 variants.
All inputs are finite; a program needn't handle non-finite values.
Results may differ from the reference program's by a relative error of at most 0.0023.
Values may be sent and summed in bfloat16 or wider, within the bound.
A program may use at most 64 MiB of HBM per device.

```python
import math
import jax
import jax.numpy as jnp
from jax import lax

SAMPLES = 768
WINDOW = 4096
SPAN = 6144
PERMS = 256
BLOCK_GENES = 128
BLOCKS = 4
GENES = 512


def draw_starts(key, part):
    drawn = jax.random.randint(key, (GENES,), 0, SPAN - WINDOW + 1, dtype=jnp.int32)
    return jnp.sort(drawn.reshape(GENES // BLOCK_GENES, BLOCK_GENES), axis=1).reshape(GENES)


def draw_genotypes(key, part):
    order_key = jax.random.fold_in(key, 11)
    shared_key = jax.random.fold_in(key, 12)
    own_key = jax.random.fold_in(key, 13)
    ranks = jax.random.permutation(order_key, BLOCKS).astype(jnp.float32)
    weights = 0.8 * ranks / max(BLOCKS - 1, 1)
    shared = jax.random.uniform(shared_key, (BLOCKS, 1, SAMPLES), dtype=jnp.float32, minval=0.0, maxval=2.0)
    own = jax.random.uniform(own_key, (BLOCKS, SPAN, SAMPLES), dtype=jnp.float32, minval=0.0, maxval=2.0)
    mixed = weights[:, None, None] * shared + (1.0 - weights[:, None, None]) * own
    return mixed.astype(jnp.bfloat16)


def steps_of(stream_key, dims, split, least, top_value):
    level, own = 1.0, jax.random.fold_in(stream_key, 6)
    for axis_at, shards_of in split:
        draws = jnp.exp(jax.random.uniform(jax.random.fold_in(own, axis_at), (shards_of,), jnp.float32, least / len(split), top_value / len(split)))
        level = level * jnp.repeat(draws, dims[axis_at] // shards_of).reshape([-1 if axis == axis_at else 1 for axis in range(len(dims))])
    return level


def bell_draw(key, dims, spread, limit, split=(), kind=jnp.bfloat16):
    values = spread * jax.random.normal(key, dims, jnp.float32)
    if split:
        values = values * steps_of(key, dims, split, -0.22, 0.18)
    return jnp.clip(values, -limit, limit).astype(kind)


def setup_inputs(seed: int = 0) -> dict:
    keys = jax.random.split(jax.random.key(seed), 5)
    return {
        "genotypes": draw_genotypes(jax.random.fold_in(keys[4], 71), 0),
        "phenotypes": bell_draw(keys[1], (GENES, SAMPLES), 1.0, 6.0, ((0, 4),), jnp.float32),
        "perm_rows": jax.vmap(lambda own: jax.random.permutation(own, SAMPLES))(jax.random.split(keys[2], PERMS)).reshape((PERMS, SAMPLES)).astype(jnp.int32),
        "starts": draw_starts(jax.random.fold_in(keys[4], 71), 0),
    }


def standard_rows(values):
    as_float = values.astype(jnp.float32)
    centred = as_float - lax.optimization_barrier(jnp.mean(as_float, axis=1, keepdims=True))
    inv_norm = lax.rsqrt(lax.optimization_barrier(jnp.sum(centred * centred, axis=1, keepdims=True)) + 1.0)
    return (centred * inv_norm).astype(jnp.bfloat16)

def reference(genotypes, phenotypes, perm_rows, starts):
    blocks = genotypes.shape[0]
    region = genotypes.shape[1]
    samples = phenotypes.shape[1]
    block_genes = phenotypes.shape[0] // blocks
    geno_std = jax.vmap(standard_rows)(genotypes)
    pheno_std = standard_rows(phenotypes).reshape(blocks, block_genes, samples)
    start_rows = starts.reshape(blocks, block_genes)
    positions = jnp.arange(region, dtype=jnp.int32)[None, :, None]
    in_window = (positions >= start_rows[:, None, :]) & (positions < start_rows[:, None, :] + WINDOW)
    perm_block = math.gcd(perm_rows.shape[0], 16)

    def per_perms(index_rows):

        def per_block(operands):
            rows_std, genes_std, window_mask = operands
            perm_table = jnp.take(genes_std.T, index_rows, axis=0)
            scores = jnp.einsum('vs,psg->vpg', rows_std.astype(jnp.float32), perm_table.astype(jnp.float32))
            return lax.optimization_barrier(jnp.max(jnp.where(window_mask[:, None, :], scores * scores, 0.0), axis=0))
        return lax.map(per_block, (geno_std, pheno_std, in_window))
    best_sq = lax.map(per_perms, perm_rows.reshape(-1, perm_block, samples))
    maxima = jnp.transpose(best_sq, (0, 2, 1, 3)).reshape(perm_rows.shape[0], blocks * block_genes) * samples
    log_stat = jnp.log1p(maxima)
    moments = jnp.stack((lax.optimization_barrier(jnp.sum(log_stat, axis=0)), lax.optimization_barrier(jnp.sum(log_stat * log_stat, axis=0)))) / perm_rows.shape[0]
    pooled = lax.optimization_barrier(jnp.sum(moments, axis=1)) / moments.shape[1]
    return (maxima, moments, pooled)
```

```python
import functools

import jax
import jax.numpy as jnp
from jax import lax
from jax.experimental import pallas as pl
from jax.experimental.pallas import tpu as pltpu
from jax.sharding import PartitionSpec as P

WINDOW = 4096
MESH = pl.DeviceIdType.MESH
GROUP = 8
PAD = 16


def standard_rows(values):
    as_float = values.astype(jnp.float32)
    centred = as_float - jnp.mean(as_float, axis=1, keepdims=True)
    inv_norm = lax.rsqrt(jnp.sum(centred * centred, axis=1, keepdims=True) + 1.0)
    return (centred * inv_norm).astype(jnp.bfloat16)


def kernel(
    sizes, geno, pheno, perms, starts, firsts, packed,
    rows, table, base, lane_starts, best, partial, inbox, others, stats,
    own_send, own_recv, far_send, far_recv, pass_send, pass_recv,
    perm_send, perm_recv, top_send, top_recv, stat_send, stat_recv,
):
    n_gene, n_var, n_perm = sizes
    n_block = n_var * n_perm
    n_all = n_block * n_gene
    chips = n_var // 2
    local, samples = geno.shape
    strips = local // PAD
    width, genes = perms.shape[0], pheno.shape[0]
    groups = genes // GROUP
    cols = width * GROUP
    lanes = lane_starts.shape[2]
    span = local * n_block
    slack = 3 * span // 4 - WINDOW
    windowed = n_var == 4 and slack >= 0 and WINDOW >= span // 2
    fat = (span - WINDOW) // (slack + 1) if windowed else 0

    gene_at = lax.axis_index("gene")
    var_at = lax.axis_index("var")
    perm_at = lax.axis_index("perm")
    core = lax.rem(var_at, 2)
    chip = var_at // 2
    here = (gene_at * n_var + var_at) * n_perm + perm_at

    def device_at(place):
        in_block = lax.rem(place, n_block)
        return {"gene": place // n_block, "var": in_block // n_perm, "perm": lax.rem(in_block, n_perm)}

    def var_of(step, core_of):
        return lax.rem(chip + step, chips) * 2 + core_of

    def place_of(var):
        if not windowed:
            return var * strips
        outer = jnp.where(var == 3, strips, 0)
        return jnp.where((var == 1) | (var == 2), 1 + (var + 1) * strips, outer)

    def first_row(var):
        return (var * n_perm + perm_at) * local

    def block(var, part=None):
        at = place_of(var)
        if part is None:
            return rows.at[pl.ds(at, strips)]
        return rows.at[pl.ds(at + part * (strips // 2), strips // 2)]

    partner = {"var": var_of(0, 1 - core)}

    barrier = pltpu.get_barrier_semaphore()
    for step in range(1, n_all):
        pl.semaphore_signal(
            barrier, inc=1, device_id=device_at(lax.rem(here + step, n_all)), device_id_type=MESH
        )

    base[...] = standard_rows(pheno[...])
    if windowed:
        rows[2 * strips] = jnp.zeros((PAD, samples), jnp.bfloat16)
    mine = block(var_at)
    for part in range(4):
        ready = standard_rows(geno[pl.ds(part * (local // 4), local // 4), :])
        mine[pl.ds(part * (strips // 4), strips // 4)] = ready.reshape(strips // 4, PAD, samples)
    best[...] = jnp.zeros_like(best)
    lane = lax.broadcasted_iota(jnp.int32, (groups, lanes), 1)
    group_line = lax.broadcasted_iota(jnp.int32, (groups, lanes), 0)
    own_lane = lane // GROUP == group_line
    spread = jnp.where(own_lane, jnp.broadcast_to(starts[...].astype(jnp.float32), (groups, lanes)), 0.0)
    shift = GROUP
    while shift < lanes:
        spread = spread + pltpu.roll(spread, shift, 1)
        shift *= 2
    lane_starts[...] = spread.astype(jnp.int32).reshape(groups, 1, lanes)

    def build(source, slot, begin, end):
        def pairs(at, carry):
            for inner in range(2):
                pair = at * 2 + inner
                placed = []
                for which in range(2):
                    order = source(pair * 2 + which).astype(jnp.int16)
                    picked = lax.broadcasted_iota(jnp.int16, (samples, samples), 0) == order
                    select = jnp.where(picked, jnp.bfloat16(1), jnp.bfloat16(0))
                    found = jnp.dot(base[...], select, preferred_element_type=jnp.float32)
                    placed.append(found.reshape(groups, GROUP, samples))
                both = jnp.concatenate(placed, axis=1).astype(jnp.bfloat16)
                table[slot, :, pl.ds(pl.multiple_of(pair * 2 * GROUP, 2 * GROUP), 2 * GROUP), :] = both
            return carry

        lax.fori_loop(begin, end, pairs, 0)

    turns = width // 4
    early = turns * 3 // 4
    build(lambda at: perms[pl.ds(at, 1), :], 0, 0, early)
    pl.semaphore_wait(barrier, n_all - 1)

    waiting = []

    def send(source, target, send_sem, recv_sem, dest=None):
        copy = pltpu.make_async_remote_copy(
            src_ref=source, dst_ref=source if dest is None else dest, send_sem=send_sem,
            recv_sem=recv_sem, device_id=target, device_id_type=MESH,
        )
        copy.start()
        return copy

    def receive(dest, recv_sem):
        pltpu.make_async_remote_copy(
            src_ref=dest, dst_ref=dest, send_sem=own_send.at[0], recv_sem=recv_sem,
            device_id=partner, device_id_type=MESH,
        ).wait_recv()

    def to_chips():
        for step in range(1, chips):
            for part in range(2):
                send(
                    block(var_at, part), {"var": var_of(step, core)},
                    far_send.at[step, part], far_recv.at[step, part],
                )

    is_mid = (var_at == 1) | (var_at == 2)
    for step in range(1, n_perm):
        waiting.append(send(
            perms, {"perm": lax.rem(perm_at + step, n_perm)},
            perm_send.at[step], perm_recv.at[step], others.at[step],
        ))
    waiting.append(send(block(var_at), partner, own_send.at[0], own_recv.at[0]))
    if windowed:
        pl.when(is_mid)(to_chips)
    else:
        to_chips()

    build(lambda at: perms[pl.ds(at, 1), :], 0, early, turns)

    def relay(step, part):
        piece = block(var_of(chips - step, core), part)
        receive(piece, far_recv.at[step, part])
        send(piece, partner, pass_send.at[step, part], pass_recv.at[step, part])

    def passed(step):
        for part in range(2):
            receive(block(var_of(chips - step, 1 - core), part), pass_recv.at[step, part])

    def relay_if(condition, part):
        pl.when(condition)(lambda: relay(1, part))

    for step in range(1, n_perm):
        receive(others.at[step], perm_recv.at[step])
        build(lambda at: others[step, pl.ds(at, 1), :], step, 0, turns)

    def top_of(values, slot, group, row):
        found = lax.dot_general(
            values, table[slot, group], (((1,), (1,)), ((), ())), preferred_element_type=jnp.float32
        )
        first = lane_starts[group]
        inside = (row >= first) & (row < first + WINDOW)
        height = values.shape[0]
        tops = []
        for piece in range(cols // lanes):
            part = found[:, piece * lanes:(piece + 1) * lanes]
            part = jnp.where(inside, part * part, 0.0)
            tops.append(jnp.max(part.reshape(height // 8, 8, lanes), axis=0))
        return jnp.concatenate(tops, axis=1)

    unroll = 4

    def score(var, begin=0, end=groups // unroll, slots=range(n_perm), unroll=unroll):
        row = first_row(var) + lax.broadcasted_iota(jnp.int32, (local, lanes), 0)
        values = block(var)

        def some(at, carry):
            for inner in range(unroll):
                group = at * unroll + inner
                for slot in slots:
                    top = top_of(values[...].reshape(local, samples), slot, group, row)
                    best[slot, group] = jnp.maximum(best[slot, group], top)
            return carry

        lax.fori_loop(begin, end, some, 0)

    def hand_over():
        for step in range(1, n_perm):
            partial[step] = jnp.max(best[step], axis=1) * samples
            waiting.append(send(
                partial.at[step], {"perm": lax.rem(perm_at + n_perm - step, n_perm)},
                top_send.at[step], top_recv.at[step], inbox.at[step],
            ))

    def strip_of(row, most):
        return lax.div(lax.min(lax.max(row, 0), most * PAD), PAD)

    def strips_at(begin, count):
        return jnp.concatenate([rows[begin + at] for at in range(count)], axis=0)

    def slide(slot):
        low = first_row(0)
        jump = first_row(3) - low - local
        height = local + PAD
        line = lax.broadcasted_iota(jnp.int32, (height, lanes), 0)

        def some(at, carry):
            for inner in range(2 * unroll):
                group = at * 2 * unroll + inner
                skip = strip_of(firsts[group * GROUP] - low, strips)
                spot = skip * PAD + line
                row = spot + low + jnp.where(spot >= local, jump, 0)
                values = strips_at(skip, strips + 1)
                top = top_of(values, slot, group, row)
                best[slot, group] = jnp.maximum(best[slot, group], top)
            return carry

        lax.fori_loop(0, groups // (2 * unroll), some, 0)

    def widen(slot):
        extent = [firsts[(group + 1) * GROUP - 1] - firsts[group * GROUP] for group in range(groups)]
        taken = [jnp.bool_(False)] * groups
        low, high = first_row(0), first_row(3)
        for place in range(fat):
            chosen, most, begin = jnp.int32(0), jnp.int32(-1), jnp.int32(0)
            for group in range(groups):
                better = jnp.logical_not(taken[group]) & (extent[group] > most)
                chosen = jnp.where(better, group, chosen)
                most = jnp.where(better, extent[group], most)
                begin = jnp.where(better, firsts[group * GROUP], begin)
            taken = [taken[group] | (chosen == group) for group in range(groups)]
            reach = (span - WINDOW) // (place + 1) - slack
            count = min(strips, (reach + 2 * PAD - 1) // PAD)
            skip = strip_of(begin - low, strips - count)
            row = high + skip * PAD + lax.broadcasted_iota(jnp.int32, (count * PAD, lanes), 0)
            values = strips_at(strips + skip, count)
            top = top_of(values, slot, chosen, row)
            for group in range(groups):
                added = jnp.where(chosen == group, top, 0.0)
                best[slot, group] = jnp.maximum(best[slot, group], added)

    if windowed:
        near_mid, near_outer = var_of(0, 1 - chip), var_of(0, chip)
        far_mid = var_of(1, chip)
        turn = groups // unroll
        is_outer = jnp.logical_not(is_mid)
        relay_if(is_outer, 0)
        pl.when(var_at != near_mid)(lambda: receive(block(near_mid), own_recv.at[0]))
        score(near_mid, 0, turn // 2)
        pl.when(is_outer)(to_chips)
        score(near_mid, turn // 2, turn * 3 // 4)
        relay_if(is_outer, 1)
        score(near_mid, turn * 3 // 4, turn)
        pl.when(is_mid)(lambda: passed(1))
        score(far_mid, 0, turn // 2)
        relay_if(is_mid, 0)
        score(far_mid, turn // 2, turn * 3 // 4)
        score(far_mid, turn * 3 // 2, turn * 2 - 1, unroll=unroll // 2)
        relay_if(is_mid, 1)
        score(far_mid, turn * 2 - 1, turn * 2, unroll=unroll // 2)
        pl.when(var_at != near_outer)(lambda: receive(block(near_outer), own_recv.at[0]))
        pl.when(is_outer)(lambda: passed(1))
        for slot in range(1, n_perm):
            slide(slot)
            widen(slot)
        hand_over()
        slide(0)
        widen(0)
    else:
        score(var_at)
        receive(block(var_of(0, 1 - core)), own_recv.at[0])
        score(var_of(0, 1 - core))
        for step in range(1, chips):
            for part in range(2):
                relay(step, part)
            score(var_of(chips - step, core))
            passed(step)
            score(var_of(chips - step, 1 - core))
        hand_over()

    partial[0] = jnp.max(best[0], axis=1) * samples
    for step in range(1, n_perm):
        receive(inbox.at[step], top_recv.at[step])
    top = partial[0]
    for step in range(1, n_perm):
        top = jnp.maximum(top, inbox[step])

    def over_perms(values):
        total = values[:, :lanes]
        for piece in range(1, cols // lanes):
            total = total + values[:, piece * lanes:(piece + 1) * lanes]
        shift = GROUP
        while shift < lanes:
            total = total + pltpu.roll(total, shift, 1)
            shift *= 2
        return jnp.sum(jnp.where(own_lane, total, 0.0), axis=0, keepdims=True)

    log_stat = jnp.log1p(top)
    stats[here, 0:1] = over_perms(log_stat)
    stats[here, 1:2] = over_perms(log_stat * log_stat)
    for step in range(1, n_all):
        waiting.append(send(
            stats.at[here], device_at(lax.rem(here + step, n_all)), stat_send.at[step], stat_recv.at[step],
        ))

    spot = lax.broadcasted_iota(jnp.int32, (cols, genes), 0)
    gene = lax.broadcasted_iota(jnp.int32, (cols, genes), 1)
    expand = jnp.where(own_lane, 1.0, 0.0)
    wide = lax.dot_general(
        top, expand, (((0,), (0,)), ((), ())), precision=lax.Precision.HIGHEST,
        preferred_element_type=jnp.float32,
    )
    wide = jnp.where(lax.rem(spot, GROUP) == lax.rem(gene, GROUP), wide, 0.0)
    packed[pl.ds(0, width), :] = jnp.sum(wide.reshape(width, GROUP, genes), axis=1)

    for step in range(1, n_all):
        receive(stats.at[lax.rem(here + n_all - step, n_all)], stat_recv.at[step])
    mean = jnp.sum(stats[pl.ds(gene_at * n_block, n_block)], axis=0) / (width * n_block)
    whole = jnp.sum(stats[...], axis=0) / (width * n_block)
    overall = jnp.sum(whole, axis=1, keepdims=True) / (genes * n_gene)
    packed[pl.ds(width, 2), :] = mean
    packed[pl.ds(width + 2, 2), :] = jnp.broadcast_to(overall, (2, genes))

    for step in range(1, chips):
        for part in range(2):
            pltpu.make_async_remote_copy(
                src_ref=block(var_at, part), dst_ref=block(var_at, part), send_sem=far_send.at[step, part],
                recv_sem=far_recv.at[step, part], device_id=partner, device_id_type=MESH,
            ).wait_send()
            pltpu.make_async_remote_copy(
                src_ref=block(var_at, part), dst_ref=block(var_at, part), send_sem=pass_send.at[step, part],
                recv_sem=pass_recv.at[step, part], device_id=partner, device_id_type=MESH,
            ).wait_send()
    for copy in waiting:
        copy.wait_send()


def unpack(packed, maxima, moments, pooled):
    width = maxima.shape[0]
    maxima[...] = packed[pl.ds(0, width), :]
    moments[...] = packed[pl.ds(width, 2), :]
    for place in range(2):
        pooled[place] = packed[width + 2 + place, 0]


def solution(mesh):
    n_gene, n_var, n_perm = (mesh.shape[name] for name in ("gene", "var", "perm"))
    n_block = n_var * n_perm
    n_all = n_block * n_gene

    def shards(genotypes, phenotypes, perm_rows, starts):
        _, local, samples = genotypes.shape
        genes = phenotypes.shape[0]
        width = perm_rows.shape[0]
        groups = genes // GROUP
        cols = width * GROUP
        chips = n_var // 2
        dma = pltpu.SemaphoreType.DMA
        vmem = pl.BlockSpec(memory_space=pltpu.VMEM)
        smem = pl.BlockSpec(memory_space=pltpu.SMEM)
        flops = 2 * width * genes * samples * (local * n_block + samples)
        packed = pl.pallas_call(
            functools.partial(kernel, (n_gene, n_var, n_perm)),
            out_shape=jax.ShapeDtypeStruct((width + 8, genes), jnp.float32),
            in_specs=[vmem] * 4 + [smem],
            out_specs=vmem,
            scratch_shapes=[
                pltpu.VMEM((n_var * local // PAD + 1, PAD, samples), jnp.bfloat16),
                pltpu.VMEM((n_perm, groups, cols, samples), jnp.bfloat16),
                pltpu.VMEM((genes, samples), jnp.bfloat16),
                pltpu.VMEM((groups, 1, genes), jnp.int32),
                pltpu.VMEM((n_perm, groups, 8, cols), jnp.float32),
                pltpu.VMEM((n_perm, groups, cols), jnp.float32),
                pltpu.VMEM((n_perm, groups, cols), jnp.float32),
                pltpu.VMEM((n_perm, width, samples), jnp.int32),
                pltpu.VMEM((n_all, 2, genes), jnp.float32),
                dma((1,)), dma((1,)), dma((chips, 2)), dma((chips, 2)), dma((chips, 2)), dma((chips, 2)),
                dma((n_perm,)), dma((n_perm,)), dma((n_perm,)), dma((n_perm,)),
                dma((n_all,)), dma((n_all,)),
            ],
            compiler_params=pltpu.CompilerParams(
                collective_id=0, has_side_effects=True, vmem_limit_bytes=56 * 1024 * 1024
            ),
            cost_estimate=pl.CostEstimate(
                flops=flops, bytes_accessed=local * samples * 2, transcendentals=0
            ),
        )(genotypes[0], phenotypes, perm_rows, starts.reshape(1, genes), starts)
        return pl.pallas_call(
            unpack,
            out_shape=(
                jax.ShapeDtypeStruct((width, genes), jnp.float32),
                jax.ShapeDtypeStruct((2, genes), jnp.float32),
                jax.ShapeDtypeStruct((2,), jnp.float32),
            ),
            in_specs=[vmem],
            out_specs=(vmem, vmem, pl.BlockSpec(memory_space=pltpu.SMEM)),
        )(packed)

    return jax.shard_map(
        shards,
        mesh=mesh,
        in_specs=(
            P("gene", ("var", "perm"), None),
            P("gene", None),
            P(("var", "perm"), None),
            P("gene"),
        ),
        out_specs=(P(("var", "perm"), "gene"), P(None, "gene"), P()),
        check_vma=False,
    )
```

```python
import functools

import jax
import jax.numpy as jnp
from jax import lax
from jax.experimental import pallas as pl
from jax.experimental.pallas import tpu as pltpu
from jax.sharding import PartitionSpec as P

WINDOW = 4096
MESH = pl.DeviceIdType.MESH
GROUP = 8
PAD = 16


def standard_rows(values):
    as_float = values.astype(jnp.float32)
    centred = as_float - jnp.mean(as_float, axis=1, keepdims=True)
    inv_norm = lax.rsqrt(jnp.sum(centred * centred, axis=1, keepdims=True) + 1.0)
    return (centred * inv_norm).astype(jnp.bfloat16)


def kernel(
    sizes, geno, pheno, perms, starts, firsts, packed,
    raw, raw_sem, rows, table, base, lane_starts, best, partial, inbox, others, stats,
    own_send, own_recv, far_send, far_recv, pass_send, pass_recv,
    perm_send, perm_recv, top_send, top_recv, stat_send, stat_recv,
):
    n_gene, n_var, n_perm = sizes
    n_block = n_var * n_perm
    n_all = n_block * n_gene
    chips = n_var // 2
    local, samples = geno.shape
    strips = local // PAD
    width, genes = perms.shape[0], pheno.shape[0]
    groups = genes // GROUP
    cols = width * GROUP
    lanes = lane_starts.shape[2]
    span = local * n_block
    slack = 3 * span // 4 - WINDOW
    windowed = n_var == 4 and slack >= 0 and WINDOW >= span // 2
    fat = (span - WINDOW) // (slack + 1) if windowed else 0

    gene_at = lax.axis_index("gene")
    var_at = lax.axis_index("var")
    perm_at = lax.axis_index("perm")
    core = lax.rem(var_at, 2)
    chip = var_at // 2
    here = (gene_at * n_var + var_at) * n_perm + perm_at

    def device_at(place):
        in_block = lax.rem(place, n_block)
        return {"gene": place // n_block, "var": in_block // n_perm, "perm": lax.rem(in_block, n_perm)}

    def var_of(step, core_of):
        return lax.rem(chip + step, chips) * 2 + core_of

    def place_of(var):
        if not windowed:
            return var * strips
        outer = jnp.where(var == 3, strips, 0)
        return jnp.where((var == 1) | (var == 2), 1 + (var + 1) * strips, outer)

    def first_row(var):
        return (var * n_perm + perm_at) * local

    def block(var, part=None):
        at = place_of(var)
        if part is None:
            return rows.at[pl.ds(at, strips)]
        return rows.at[pl.ds(at + part * (strips // 2), strips // 2)]

    partner = {"var": var_of(0, 1 - core)}

    fetch = pltpu.make_async_copy(geno, raw, raw_sem)
    fetch.start()
    barrier = pltpu.get_barrier_semaphore()
    for step in range(1, n_all):
        pl.semaphore_signal(
            barrier, inc=1, device_id=device_at(lax.rem(here + step, n_all)), device_id_type=MESH
        )

    base[...] = standard_rows(pheno[...])
    best[...] = jnp.zeros_like(best)
    lane = lax.broadcasted_iota(jnp.int32, (groups, lanes), 1)
    group_line = lax.broadcasted_iota(jnp.int32, (groups, lanes), 0)
    own_lane = lane // GROUP == group_line
    spread = jnp.where(own_lane, jnp.broadcast_to(starts[...].astype(jnp.float32), (groups, lanes)), 0.0)
    shift = GROUP
    while shift < lanes:
        spread = spread + pltpu.roll(spread, shift, 1)
        shift *= 2
    lane_starts[...] = spread.astype(jnp.int32).reshape(groups, 1, lanes)

    def build(source, slot, begin, end):
        def pairs(at, carry):
            for inner in range(2):
                pair = at * 2 + inner
                placed = []
                for which in range(2):
                    order = source(pair * 2 + which).astype(jnp.int16)
                    picked = lax.broadcasted_iota(jnp.int16, (samples, samples), 0) == order
                    select = jnp.where(picked, jnp.bfloat16(1), jnp.bfloat16(0))
                    found = jnp.dot(base[...], select, preferred_element_type=jnp.float32)
                    placed.append(found.reshape(groups, GROUP, samples))
                both = jnp.concatenate(placed, axis=1).astype(jnp.bfloat16)
                table[slot, :, pl.ds(pl.multiple_of(pair * 2 * GROUP, 2 * GROUP), 2 * GROUP), :] = both
            return carry

        lax.fori_loop(begin, end, pairs, 0)

    turns = width // 4
    early = turns // 2
    build(lambda at: perms[pl.ds(at, 1), :], 0, 0, early)
    if windowed:
        rows[2 * strips] = jnp.zeros((PAD, samples), jnp.bfloat16)
    mine = block(var_at)
    fetch.wait()
    for part in range(4):
        ready = standard_rows(raw[pl.ds(part * (local // 4), local // 4), :])
        mine[pl.ds(part * (strips // 4), strips // 4)] = ready.reshape(strips // 4, PAD, samples)
    pl.semaphore_wait(barrier, n_all - 1)

    waiting = []

    def send(source, target, send_sem, recv_sem, dest=None):
        copy = pltpu.make_async_remote_copy(
            src_ref=source, dst_ref=source if dest is None else dest, send_sem=send_sem,
            recv_sem=recv_sem, device_id=target, device_id_type=MESH,
        )
        copy.start()
        return copy

    def receive(dest, recv_sem):
        pltpu.make_async_remote_copy(
            src_ref=dest, dst_ref=dest, send_sem=own_send.at[0], recv_sem=recv_sem,
            device_id=partner, device_id_type=MESH,
        ).wait_recv()

    def to_chips():
        for step in range(1, chips):
            for part in range(2):
                send(
                    block(var_at, part), {"var": var_of(step, core)},
                    far_send.at[step, part], far_recv.at[step, part],
                )

    is_mid = (var_at == 1) | (var_at == 2)
    for step in range(1, n_perm):
        waiting.append(send(
            perms, {"perm": lax.rem(perm_at + step, n_perm)},
            perm_send.at[step], perm_recv.at[step], others.at[step],
        ))
    waiting.append(send(block(var_at), partner, own_send.at[0], own_recv.at[0]))
    if windowed:
        pl.when(is_mid)(to_chips)
    else:
        to_chips()

    build(lambda at: perms[pl.ds(at, 1), :], 0, early, turns)

    def relay(step, part):
        piece = block(var_of(chips - step, core), part)
        receive(piece, far_recv.at[step, part])
        send(piece, partner, pass_send.at[step, part], pass_recv.at[step, part])

    def passed(step):
        for part in range(2):
            receive(block(var_of(chips - step, 1 - core), part), pass_recv.at[step, part])

    def relay_if(condition, part):
        pl.when(condition)(lambda: relay(1, part))

    def build_others():
        for step in range(1, n_perm):
            receive(others.at[step], perm_recv.at[step])
            build(lambda at: others[step, pl.ds(at, 1), :], step, 0, turns)

    def top_of(values, slot, group, row):
        found = lax.dot_general(
            values, table[slot, group], (((1,), (1,)), ((), ())), preferred_element_type=jnp.float32
        )
        first = lane_starts[group]
        inside = (row >= first) & (row < first + WINDOW)
        height = values.shape[0]
        tops = []
        for piece in range(cols // lanes):
            part = found[:, piece * lanes:(piece + 1) * lanes]
            part = jnp.where(inside, part * part, 0.0)
            tops.append(jnp.max(part.reshape(height // 8, 8, lanes), axis=0))
        return jnp.concatenate(tops, axis=1)

    unroll = 4

    def score(var, begin=0, end=groups // unroll, slots=range(n_perm), unroll=unroll):
        row = first_row(var) + lax.broadcasted_iota(jnp.int32, (local, lanes), 0)
        values = block(var)

        def some(at, carry):
            for inner in range(unroll):
                group = at * unroll + inner
                for slot in slots:
                    top = top_of(values[...].reshape(local, samples), slot, group, row)
                    best[slot, group] = jnp.maximum(best[slot, group], top)
            return carry

        lax.fori_loop(begin, end, some, 0)

    def hand_over():
        for step in range(1, n_perm):
            partial[step] = jnp.max(best[step], axis=1) * samples
            waiting.append(send(
                partial.at[step], {"perm": lax.rem(perm_at + n_perm - step, n_perm)},
                top_send.at[step], top_recv.at[step], inbox.at[step],
            ))

    def strip_of(row, most):
        return lax.div(lax.min(lax.max(row, 0), most * PAD), PAD)

    def strips_at(begin, count):
        return jnp.concatenate([rows[begin + at] for at in range(count)], axis=0)

    def slide(slot):
        low = first_row(0)
        jump = first_row(3) - low - local
        height = local + PAD
        line = lax.broadcasted_iota(jnp.int32, (height, lanes), 0)

        def some(at, carry):
            for inner in range(2 * unroll):
                group = at * 2 * unroll + inner
                skip = strip_of(firsts[group * GROUP] - low, strips)
                spot = skip * PAD + line
                row = spot + low + jnp.where(spot >= local, jump, 0)
                values = strips_at(skip, strips + 1)
                top = top_of(values, slot, group, row)
                best[slot, group] = jnp.maximum(best[slot, group], top)
            return carry

        lax.fori_loop(0, groups // (2 * unroll), some, 0)

    def widest():
        extent = [firsts[(group + 1) * GROUP - 1] - firsts[group * GROUP] for group in range(groups)]
        taken = [jnp.bool_(False)] * groups
        found = []
        for place in range(fat):
            chosen, most, begin = jnp.int32(0), jnp.int32(-1), jnp.int32(0)
            for group in range(groups):
                better = jnp.logical_not(taken[group]) & (extent[group] > most)
                chosen = jnp.where(better, group, chosen)
                most = jnp.where(better, extent[group], most)
                begin = jnp.where(better, firsts[group * GROUP], begin)
            taken = [taken[group] | (chosen == group) for group in range(groups)]
            found.append((chosen, begin))
        return found

    def widen(slot, found):
        low, high = first_row(0), first_row(3)
        tops = []
        for place, (chosen, begin) in enumerate(found):
            reach = (span - WINDOW) // (place + 1) - slack
            count = min(strips, (reach + 2 * PAD - 1) // PAD)
            skip = strip_of(begin - low, strips - count)
            row = high + skip * PAD + lax.broadcasted_iota(jnp.int32, (count * PAD, lanes), 0)
            tops.append(top_of(strips_at(strips + skip, count), slot, chosen, row))
        for group in range(groups):
            added = best[slot, group]
            for (chosen, _), top in zip(found, tops):
                added = jnp.maximum(added, jnp.where(chosen == group, top, 0.0))
            best[slot, group] = added

    if windowed:
        near_mid, near_outer = var_of(0, 1 - chip), var_of(0, chip)
        far_mid = var_of(1, chip)
        turn = groups // unroll
        is_outer = jnp.logical_not(is_mid)
        pl.when(var_at != near_mid)(lambda: receive(block(near_mid), own_recv.at[0]))
        score(near_mid, 0, turn // 2, range(1), 2 * unroll)
        build_others()
        pl.when(is_outer)(to_chips)
        relay_if(is_outer, 0)
        score(near_mid, 0, turn // 4, range(1, n_perm), 2 * unroll)
        relay_if(is_outer, 1)
        score(near_mid, turn // 4, turn // 2, range(1, n_perm), 2 * unroll)
        pl.when(is_mid)(lambda: passed(1))
        score(far_mid, 0, turn // 2)
        relay_if(is_mid, 0)
        score(far_mid, turn // 2, turn * 3 // 4)
        score(far_mid, turn * 3 // 2, turn * 2 - 1, unroll=unroll // 2)
        relay_if(is_mid, 1)
        score(far_mid, turn * 2 - 1, turn * 2, unroll=unroll // 2)
        pl.when(var_at != near_outer)(lambda: receive(block(near_outer), own_recv.at[0]))
        pl.when(is_outer)(lambda: passed(1))
        found = widest()
        for slot in range(1, n_perm):
            slide(slot)
            widen(slot, found)
        hand_over()
        slide(0)
        widen(0, found)
    else:
        build_others()
        score(var_at)
        receive(block(var_of(0, 1 - core)), own_recv.at[0])
        score(var_of(0, 1 - core))
        for step in range(1, chips):
            for part in range(2):
                relay(step, part)
            score(var_of(chips - step, core))
            passed(step)
            score(var_of(chips - step, 1 - core))
        hand_over()

    partial[0] = jnp.max(best[0], axis=1) * samples
    for step in range(1, n_perm):
        receive(inbox.at[step], top_recv.at[step])
    top = partial[0]
    for step in range(1, n_perm):
        top = jnp.maximum(top, inbox[step])

    def over_perms(values):
        total = values[:, :lanes]
        for piece in range(1, cols // lanes):
            total = total + values[:, piece * lanes:(piece + 1) * lanes]
        shift = GROUP
        while shift < lanes:
            total = total + pltpu.roll(total, shift, 1)
            shift *= 2
        return jnp.sum(jnp.where(own_lane, total, 0.0), axis=0, keepdims=True)

    log_stat = jnp.log1p(top)
    stats[here, 0:1] = over_perms(log_stat)
    stats[here, 1:2] = over_perms(log_stat * log_stat)
    for step in range(1, n_all):
        waiting.append(send(
            stats.at[here], device_at(lax.rem(here + step, n_all)), stat_send.at[step], stat_recv.at[step],
        ))

    spot = lax.broadcasted_iota(jnp.int32, (cols, genes), 0)
    gene = lax.broadcasted_iota(jnp.int32, (cols, genes), 1)
    expand = jnp.where(own_lane, 1.0, 0.0)
    wide = lax.dot_general(
        top, expand, (((0,), (0,)), ((), ())), precision=lax.Precision.HIGHEST,
        preferred_element_type=jnp.float32,
    )
    wide = jnp.where(lax.rem(spot, GROUP) == lax.rem(gene, GROUP), wide, 0.0)
    packed[pl.ds(0, width), :] = jnp.sum(wide.reshape(width, GROUP, genes), axis=1)

    for step in range(1, n_all):
        receive(stats.at[lax.rem(here + n_all - step, n_all)], stat_recv.at[step])
    mean = jnp.sum(stats[pl.ds(gene_at * n_block, n_block)], axis=0) / (width * n_block)
    whole = jnp.sum(stats[...], axis=0) / (width * n_block)
    overall = jnp.sum(whole, axis=1, keepdims=True) / (genes * n_gene)
    packed[pl.ds(width, 2), :] = mean
    packed[pl.ds(width + 2, 2), :] = jnp.broadcast_to(overall, (2, genes))

    for step in range(1, chips):
        for part in range(2):
            pltpu.make_async_remote_copy(
                src_ref=block(var_at, part), dst_ref=block(var_at, part), send_sem=far_send.at[step, part],
                recv_sem=far_recv.at[step, part], device_id=partner, device_id_type=MESH,
            ).wait_send()
            pltpu.make_async_remote_copy(
                src_ref=block(var_at, part), dst_ref=block(var_at, part), send_sem=pass_send.at[step, part],
                recv_sem=pass_recv.at[step, part], device_id=partner, device_id_type=MESH,
            ).wait_send()
    for copy in waiting:
        copy.wait_send()


def unpack(packed, maxima, moments, pooled):
    width = maxima.shape[0]
    maxima[...] = packed[pl.ds(0, width), :]
    moments[...] = packed[pl.ds(width, 2), :]
    for place in range(2):
        pooled[place] = packed[width + 2 + place, 0]


def solution(mesh):
    n_gene, n_var, n_perm = (mesh.shape[name] for name in ("gene", "var", "perm"))
    n_block = n_var * n_perm
    n_all = n_block * n_gene

    def shards(genotypes, phenotypes, perm_rows, starts):
        _, local, samples = genotypes.shape
        genes = phenotypes.shape[0]
        width = perm_rows.shape[0]
        groups = genes // GROUP
        cols = width * GROUP
        chips = n_var // 2
        dma = pltpu.SemaphoreType.DMA
        vmem = pl.BlockSpec(memory_space=pltpu.VMEM)
        smem = pl.BlockSpec(memory_space=pltpu.SMEM)
        flops = 2 * width * genes * samples * (local * n_block + samples)
        packed = pl.pallas_call(
            functools.partial(kernel, (n_gene, n_var, n_perm)),
            out_shape=jax.ShapeDtypeStruct((width + 8, genes), jnp.float32),
            in_specs=[pl.BlockSpec(memory_space=pl.ANY)] + [vmem] * 3 + [smem],
            out_specs=vmem,
            scratch_shapes=[
                pltpu.VMEM((local, samples), jnp.bfloat16), dma,
                pltpu.VMEM((n_var * local // PAD + 1, PAD, samples), jnp.bfloat16),
                pltpu.VMEM((n_perm, groups, cols, samples), jnp.bfloat16),
                pltpu.VMEM((genes, samples), jnp.bfloat16),
                pltpu.VMEM((groups, 1, genes), jnp.int32),
                pltpu.VMEM((n_perm, groups, 8, cols), jnp.float32),
                pltpu.VMEM((n_perm, groups, cols), jnp.float32),
                pltpu.VMEM((n_perm, groups, cols), jnp.float32),
                pltpu.VMEM((n_perm, width, samples), jnp.int32),
                pltpu.VMEM((n_all, 2, genes), jnp.float32),
                dma((1,)), dma((1,)), dma((chips, 2)), dma((chips, 2)), dma((chips, 2)), dma((chips, 2)),
                dma((n_perm,)), dma((n_perm,)), dma((n_perm,)), dma((n_perm,)),
                dma((n_all,)), dma((n_all,)),
            ],
            compiler_params=pltpu.CompilerParams(
                collective_id=0, has_side_effects=True, vmem_limit_bytes=56 * 1024 * 1024
            ),
            cost_estimate=pl.CostEstimate(
                flops=flops, bytes_accessed=local * samples * 2, transcendentals=0
            ),
        )(genotypes[0], phenotypes, perm_rows, starts.reshape(1, genes), starts)
        return pl.pallas_call(
            unpack,
            out_shape=(
                jax.ShapeDtypeStruct((width, genes), jnp.float32),
                jax.ShapeDtypeStruct((2, genes), jnp.float32),
                jax.ShapeDtypeStruct((2,), jnp.float32),
            ),
            in_specs=[vmem],
            out_specs=(vmem, vmem, pl.BlockSpec(memory_space=pltpu.SMEM)),
        )(packed)

    return jax.shard_map(
        shards,
        mesh=mesh,
        in_specs=(
            P("gene", ("var", "perm"), None),
            P("gene", None),
            P(("var", "perm"), None),
            P("gene"),
        ),
        out_specs=(P(("var", "perm"), "gene"), P(None, "gene"), P()),
        check_vma=False,
    )
```
